256 devices in a mesh: orig: 32 (over z, x), link: 8 (over y, core).
Axes of the slice: x: 4, y: 4, z: 8, core: 2. Of those that a mesh axis runs over, the one named last changes fastest.
Arguments:
- flows: float32 [3072], P('link'), may hold values from 0.2 to 2
- free_time: float32 [3072], P('link'), may hold values from 0.5 to 4
- capacity: float32 [3072], P('link'), may hold values from 0.5 to 2
- path_links: int32 [24, 1048576], P(None, ('orig', 'link')), may hold values from 0 to 3071, as said below
- demand: float32 [262144], P(('orig', 'link')), may hold values from 0.00012207031 to 0.0012207031
- chosen: int32 [262144], P(('orig', 'link')), may hold values from 0 to 3
Outputs:
- path_costs: float32 [1048576], P(('orig', 'link'))
- new_flows: float32 [3072], P('link')
The draws below stay inside these ranges and needn't reach their ends.
Inputs may be any that keep to these rules, and one draw needn't show every extreme that they name: `path_links`: each entry is a link number; a path that names a link twice uses it twice. Pair k chooses path 4 * k + chosen[k].
All inputs are finite; a program needn't handle non-finite values.
Results may differ from the reference program's by a relative error of at most 0.00011.
Values sent between devices are 32-bit elements; how exact they have to be, the bound alone decides.
A program may use at most 128 MiB of HBM per device.

```python
import math
import jax
import jax.numpy as jnp

L = 3072
HOPS = 24
PER_OD = 4
LINE_STEPS = 8
PATH_DEV = 4096
PATHS = 1048576
ODS = 262144


def draw_path_links(key, part):
    blocks = PATHS // PATH_DEV
    center_key = jax.random.fold_in(key, 11)
    offset_key = jax.random.fold_in(key, 12)
    centers = jax.random.randint(center_key, (blocks,), 0, L, dtype=jnp.int32)
    offsets = jax.random.randint(offset_key, (HOPS, PATHS), 0, L // 8, dtype=jnp.int32)
    starts = jnp.repeat(centers, PATH_DEV, total_repeat_length=PATHS)
    return (starts[None, :] + offsets) % L


def plant(array, stream_key, low, high):
    spot = [jax.random.randint(jax.random.fold_in(stream_key, axis), (), 0, length) for axis, length in enumerate(array.shape)]
    main_axis = array.shape.index(max(array.shape))
    next_to = spot[:main_axis] + [(spot[main_axis] + 1) % array.shape[main_axis]] + spot[main_axis + 1:]
    return array.at[tuple(spot)].set(low).at[tuple(next_to)].set(high)


def levels(rng, shape, shards, low, largest):
    loudness, own = 1.0, jax.random.fold_in(rng, 6)
    for dim, shards_of in shards:
        steps = jnp.exp(jax.random.uniform(jax.random.fold_in(own, dim), (shards_of,), jnp.float32, low / len(shards), largest / len(shards)))
        loudness = loudness * jnp.repeat(steps, shape[dim] // shards_of).reshape([-1 if axis == dim else 1 for axis in range(len(shape))])
    return loudness


def setup_inputs(seed: int = 0) -> dict:
    key_list = jax.random.split(jax.random.key(seed), 7)
    return {
        "flows": jnp.clip(0.2 + 1.8 * jax.random.uniform(key_list[0], (L,), jnp.float32) ** levels(key_list[0], (L,), ((0, 8),), -0.2, 0.2), 0.2, 2.0),
        "free_time": jnp.clip(jnp.exp(math.log(4.0) - 2.0794415 * jax.random.uniform(key_list[1], (L,), jnp.float32) ** levels(key_list[1], (L,), ((0, 8),), -0.2, 0.2)), 0.5, 4.0),
        "capacity": jnp.clip(jnp.exp(math.log(2.0) - 1.3862944 * jax.random.uniform(key_list[2], (L,), jnp.float32) ** levels(key_list[2], (L,), ((0, 8),), -0.2, 0.2)), 0.5, 2.0),
        "path_links": draw_path_links(jax.random.fold_in(key_list[6], 71), 0),
        "demand": jnp.clip(jnp.exp(math.log(0.0012207031) - 2.3025851 * jax.random.uniform(key_list[4], (ODS,), jnp.float32) ** levels(key_list[4], (ODS,), ((0, 256),), -0.2, 0.2)), 0.00012207031, 0.0012207031),
        "chosen": plant(jax.random.randint(key_list[5], (ODS,), 0, PER_OD), jax.random.fold_in(key_list[5], 1), 0, PER_OD - 1).astype(jnp.int32),
    }


def travel(volume, free_time, capacity):
    ratio = volume / capacity
    square = ratio * ratio
    return free_time * (1.0 + 0.15 * square * square)


def reference(flows, free_time, capacity, path_links, demand, chosen):
    times = travel(flows, free_time, capacity)
    path_costs = jnp.sum(times[path_links], axis=0)
    grouped = path_links.reshape(HOPS, ODS, PER_OD)
    picked = jnp.take_along_axis(grouped, chosen.astype(jnp.int32)[None, :, None], axis=2)[:, :, 0]
    weights = jnp.broadcast_to(demand[None, :], picked.shape).reshape(-1)
    loads = jax.ops.segment_sum(weights, picked.reshape(-1), num_segments=L)
    direction = loads - flows
    alpha = jnp.float32(0.5)
    for step in range(LINE_STEPS):
        volume = flows + alpha * direction
        ratio = volume / capacity
        square = ratio * ratio
        slope = jnp.sum(free_time * (1.0 + 0.15 * square * square) * direction)
        curve = jnp.sum(free_time / capacity * direction * direction * (1.0 + 0.6 * square * square))
        alpha = alpha - slope / curve
    new_flows = flows + alpha * direction
    return path_costs, new_flows
```

```python
import functools

import jax
import jax.numpy as jnp
from jax import lax
from jax.experimental import pallas as pl
from jax.experimental.pallas import tpu as pltpu
from jax.sharding import PartitionSpec as P

PER_OD = 4
LINE_STEPS = 8
LANES = 128
MESH = pl.DeviceIdType.MESH


def travel(volume, free_time, capacity):
    ratio = volume / capacity
    square = ratio * ratio
    return free_time * (1.0 + 0.15 * square * square)


def gathered(table, index):
    return jnp.take_along_axis(table, index, axis=1, mode="promise_in_bounds")


def kernel(
    links_hbm,
    chosen_hbm,
    demand_hbm,
    flows_hbm,
    free_hbm,
    cap_hbm,
    costs_ref,
    new_ref,
    links,
    chosen,
    demand,
    flows,
    free,
    cap,
    part,
    recv,
    sums,
    terms,
    table,
    local_sem,
    time_send,
    time_recv,
    part_send,
    part_recv,
    sum_send,
    sum_recv,
    term_send,
    term_recv,
):
    hops, paths = links.shape
    rows = table.shape[1]
    n_link = table.shape[0]
    n_orig = sums.shape[0]
    n_rows = n_link * rows
    me_link = lax.axis_index("link")
    me_orig = lax.axis_index("orig")

    loads_in = [
        pltpu.make_async_copy(src, dst, local_sem.at[k])
        for k, (src, dst) in enumerate(
            (
                (chosen_hbm, chosen),
                (links_hbm, links),
                (demand_hbm, demand),
                (flows_hbm, flows),
                (free_hbm, free),
                (cap_hbm, cap),
            )
        )
    ]
    for copy in loads_in:
        copy.start()

    barrier = pltpu.get_barrier_semaphore()
    for d in range(1, n_link):
        pl.semaphore_signal(
            barrier, inc=1, device_id=(me_orig, (me_link + d) % n_link), device_id_type=MESH
        )
    for d in range(1, n_orig):
        pl.semaphore_signal(
            barrier, inc=1, device_id=((me_orig + d) % n_orig, me_link), device_id_type=MESH
        )

    for copy in loads_in:
        copy.wait()

    table[me_link] = travel(flows[...], free[...], cap[...])

    lane = lax.broadcasted_iota(jnp.int32, (8, LANES), 1)
    quarter = lane // (LANES // PER_OD)
    first = (lane * PER_OD) % LANES
    low_ids = lax.broadcasted_iota(jnp.int32, (LANES, LANES), 0).astype(jnp.int16)
    row_ids = lax.broadcasted_iota(jnp.int32, (2 * n_rows, LANES), 0)
    coarse = row_ids < n_rows
    high_ids = jnp.where(coarse, row_ids, row_ids - n_rows).astype(jnp.int16)

    def block(b, total):
        start = pl.multiple_of(b * (PER_OD * LANES), PER_OD * LANES)
        where_to = first + chosen[pl.ds(b, 1), :]
        weight = demand[pl.ds(b, 1), :]
        upper = weight.astype(jnp.bfloat16).astype(jnp.float32)
        both = jnp.where(coarse, upper, weight - upper).astype(jnp.bfloat16)
        picked = []
        for g in range(hops // 8):
            group = None
            for q in range(PER_OD):
                found = gathered(
                    links[8 * g : 8 * g + 8, pl.ds(start + q * LANES, LANES)], where_to
                )
                group = found if q == 0 else jnp.where(quarter == q, found, group)
            picked.append(group)
        picked = jnp.concatenate(picked, axis=0)
        high = picked // LANES
        low = picked % LANES
        for h in range(0, hops, 2):
            lefts, rights = [], []
            for k in (h, h + 1):
                hi = jnp.broadcast_to(high[k : k + 1], (2 * n_rows, LANES)).astype(jnp.int16)
                lo = jnp.broadcast_to(low[k : k + 1], (LANES, LANES)).astype(jnp.int16)
                lefts.append(jnp.where(hi == high_ids, both, jnp.bfloat16(0)))
                rights.append(
                    jnp.where(lo == low_ids, jnp.bfloat16(1), jnp.bfloat16(0))
                )
            total = total + lax.dot_general(
                jnp.concatenate(lefts, axis=1),
                jnp.concatenate(rights, axis=1),
                (((1,), (1,)), ((), ())),
                preferred_element_type=jnp.float32,
            )
        return total

    total = lax.fori_loop(
        0,
        chosen.shape[0],
        block,
        jnp.zeros((2 * n_rows, LANES), jnp.float32),
    )
    total = total[:n_rows] + total[n_rows:]
    for k in range(n_link):
        part[k] = total[k * rows : (k + 1) * rows]

    pl.semaphore_wait(barrier, n_link + n_orig - 2)

    def to_link(src, dst, send, recv_sem, d):
        return pltpu.make_async_remote_copy(
            src_ref=src,
            dst_ref=dst,
            send_sem=send.at[d],
            recv_sem=recv_sem.at[d],
            device_id=(me_orig, (me_link + d) % n_link),
            device_id_type=MESH,
        )

    waits = []
    part_copies = [
        to_link(part.at[(me_link + d) % n_link], recv.at[me_link], part_send, part_recv, d)
        for d in range(1, n_link)
    ]
    time_copies = [
        to_link(table.at[me_link], table.at[me_link], time_send, time_recv, d)
        for d in range(1, n_link)
    ]
    for copy in part_copies:
        copy.start()
    for copy in time_copies:
        copy.start()
    recv[me_link] = part[me_link]
    for copy in part_copies:
        copy.wait_recv()
    partial = recv[0]
    for k in range(1, n_link):
        partial = partial + recv[k]
    sums[me_orig] = partial

    sum_copies = [
        pltpu.make_async_remote_copy(
            src_ref=sums.at[me_orig],
            dst_ref=sums.at[me_orig],
            send_sem=sum_send.at[d],
            recv_sem=sum_recv.at[d],
            device_id=((me_orig + d) % n_orig, me_link),
            device_id_type=MESH,
        )
        for d in range(1, n_orig)
    ]
    for copy in sum_copies:
        copy.start()

    for copy in time_copies:
        copy.wait_recv()
    times = [
        jnp.broadcast_to(table[r // rows, pl.ds(r % rows, 1), :], (8, LANES))
        for r in range(n_rows)
    ]

    def costs(b, carry):
        start = pl.multiple_of(b * LANES, LANES)
        total = jnp.zeros((8, LANES), jnp.float32)
        for g in range(hops // 8):
            index = links[8 * g : 8 * g + 8, pl.ds(start, LANES)]
            high = index // LANES
            low = index % LANES
            value = gathered(times[0], low)
            for r in range(1, n_rows):
                value = jnp.where(high == r, gathered(times[r], low), value)
            total = total + value
        costs_ref[pl.ds(b, 1), :] = jnp.sum(total, axis=0, keepdims=True)
        return carry

    lax.fori_loop(0, paths // LANES, costs, 0)

    for copy in sum_copies:
        copy.wait_recv()
    loads = sums[0]
    for k in range(1, n_orig):
        loads = loads + sums[k]
    flow = flows[...]
    direction = loads - flow

    inverse = 1.0 / cap[...]
    p = flow * inverse
    q = direction * inverse
    pp, pq, qq = p * p, p * q, q * q
    powers = (pp * pp, 4.0 * pp * pq, 6.0 * pp * qq, 4.0 * pq * qq, qq * qq)
    slope_one = free[...] * direction
    curve_one = slope_one * q
    coefficients = []
    for one, factor in ((slope_one, 0.15), (curve_one, 0.6)):
        scaled = factor * one
        for k, power in enumerate(powers):
            term = scaled * power
            coefficients.append(one + term if k == 0 else term)
    spot = lax.broadcasted_iota(jnp.int32, (rows, LANES), 1)
    packed = jnp.zeros((rows, LANES), jnp.float32)
    for k, term in enumerate(coefficients):
        packed = jnp.where(spot == k, jnp.sum(term, axis=1, keepdims=True), packed)
    terms[me_link] = packed
    term_copies = [
        to_link(terms.at[me_link], terms.at[me_link], term_send, term_recv, d)
        for d in range(1, n_link)
    ]
    for copy in term_copies:
        copy.start()
    for copy in part_copies + time_copies + sum_copies:
        copy.wait_send()
    for copy in term_copies:
        copy.wait_recv()
    whole = terms[0]
    for k in range(1, n_link):
        whole = whole + terms[k]
    whole = jnp.sum(whole, axis=0, keepdims=True)
    count = len(coefficients)
    c = [
        jnp.sum(jnp.where(spot[:1] == k, whole, 0.0), axis=1, keepdims=True)
        for k in range(count)
    ]
    s, u = c[: count // 2], c[count // 2 :]
    alpha = jnp.full((1, 1), 0.5, jnp.float32)
    for step in range(LINE_STEPS):
        slope, curve = s[-1], u[-1]
        for k in range(len(s) - 2, -1, -1):
            slope = slope * alpha + s[k]
            curve = curve * alpha + u[k]
        alpha = alpha - slope / curve
    new_ref[...] = flow + alpha * direction
    for copy in term_copies:
        copy.wait_send()


def local(n_orig, n_link, flows, free_time, capacity, path_links, demand, chosen):
    rows = flows.shape[0] // LANES
    hops, paths = path_links.shape
    pairs = demand.shape[0] // LANES
    f32 = jnp.float32
    any_space = pl.BlockSpec(memory_space=pl.ANY)
    vmem = pl.BlockSpec(memory_space=pltpu.VMEM)
    dma = pltpu.SemaphoreType.DMA
    costs, new = pl.pallas_call(
        kernel,
        out_shape=(
            jax.ShapeDtypeStruct((paths // LANES, LANES), f32),
            jax.ShapeDtypeStruct((rows, LANES), f32),
        ),
        in_specs=[any_space] * 6,
        out_specs=(vmem, vmem),
        scratch_shapes=[
            pltpu.VMEM((hops, paths), jnp.int32),
            pltpu.VMEM((pairs, LANES), jnp.int32),
            pltpu.VMEM((pairs, LANES), f32),
            pltpu.VMEM((rows, LANES), f32),
            pltpu.VMEM((rows, LANES), f32),
            pltpu.VMEM((rows, LANES), f32),
            pltpu.VMEM((n_link, rows, LANES), f32),
            pltpu.VMEM((n_link, rows, LANES), f32),
            pltpu.VMEM((n_orig, rows, LANES), f32),
            pltpu.VMEM((n_link, rows, LANES), f32),
            pltpu.VMEM((n_link, rows, LANES), f32),
            dma((6,)),
            dma((n_link,)),
            dma((n_link,)),
            dma((n_link,)),
            dma((n_link,)),
            dma((n_orig,)),
            dma((n_orig,)),
            dma((n_link,)),
            dma((n_link,)),
        ],
        compiler_params=pltpu.CompilerParams(collective_id=0, has_side_effects=True),
    )(
        path_links,
        chosen.reshape(pairs, LANES),
        demand.reshape(pairs, LANES),
        flows.reshape(rows, LANES),
        free_time.reshape(rows, LANES),
        capacity.reshape(rows, LANES),
    )
    return costs.reshape(paths), new.reshape(rows * LANES)


def solution(mesh):
    return jax.shard_map(
        functools.partial(local, mesh.shape["orig"], mesh.shape["link"]),
        mesh=mesh,
        in_specs=(
            P("link"),
            P("link"),
            P("link"),
            P(None, ("orig", "link")),
            P(("orig", "link")),
            P(("orig", "link")),
        ),
        out_specs=(P(("orig", "link")), P("link")),
        check_vma=False,
    )
```
